32 devices in a mesh: row: 8 (over z, y), col: 4 (over x, core).
Axes of the slice: x: 2, y: 2, z: 4, core: 2. Of those that a mesh axis runs over, the one named last changes fastest.
Arguments:
- densities: bfloat16 [4608, 3072], P(('row', 'col')), may hold values from -0.796875 to 0.796875
- counts: int32 [512], P(('row', 'col')), may hold values from 3 to 9
- coulomb: float32 [3072], replicated, may hold values from 0.05 to 1
- energies: float32 [4608], P(('row', 'col')), may hold values from 8 to 64
- vectors: bfloat16 [4608, 64], P(('row', 'col')), may hold values from -0.09375 to 0.09375
Outputs:
- kernel: float32 [4608, 4608], P('row', 'col')
- product: float32 [4608, 64], P(('row', 'col'))
The draws below stay inside these ranges and needn't reach their ends.
All inputs are finite; a program needn't handle non-finite values.
Results may differ from the reference program's by a relative error of at most 0.0095.
Values may be sent and summed in bfloat16 or wider, within the bound.
A program may use at most 128 MiB of HBM per device.

```python
import math
import jax
import jax.numpy as jnp
from jax import lax

G = 3072
NV = 64
SLOT = 9
K_DEV = 16
NK = 512
ROWS = 4608
N_ROW = 8
N_COL = 4


def set_ends(values, own_key, low, largest):
    spot = [jax.random.randint(jax.random.fold_in(own_key, axis), (), 0, length) for axis, length in enumerate(values.shape)]
    main_axis = values.shape.index(max(values.shape))
    beside = spot[:main_axis] + [(spot[main_axis] + 1) % values.shape[main_axis]] + spot[main_axis + 1:]
    return values.at[tuple(spot)].set(low).at[tuple(beside)].set(largest)


def levels(rng, shape, split, smallest, high):
    def one(position, shards_of):
        heights = jax.random.uniform(jax.random.fold_in(jax.random.fold_in(rng, 6), position), (shards_of,), jnp.float32, smallest / len(split), high / len(split))
        return jnp.repeat(jnp.exp(heights), shape[position] // shards_of).reshape((-1,) + (1,) * (len(shape) - position - 1))

    gain = one(*split[0])
    for cut in split[1:]:
        gain = gain * one(*cut)
    return gain


def noise(rng, dims, deviation, reach, shards=(), dtype=jnp.bfloat16):
    array = deviation * jax.random.normal(rng, dims, jnp.float32)
    if shards:
        array = array * levels(rng, dims, shards, -0.22, 0.18)
    return jnp.clip(array, -reach, reach).astype(dtype)


def setup_inputs(seed: int = 0) -> dict:
    seeds = jax.random.split(jax.random.key(seed), 6)
    densities = noise(seeds[0], (ROWS, G), 0.134, 0.796875, ((0, 32),))
    counts = set_ends(jax.random.randint(seeds[1], (NK,), 3, 10), jax.random.fold_in(seeds[1], 1), 3, 9).astype(jnp.int32)
    coulomb = jnp.clip(jnp.exp(jax.random.uniform(seeds[2], (G,), jnp.float32, math.log(0.05), math.log(1.0))), 0.05, 1.0)
    energies = jnp.clip(jnp.exp(math.log(64.0) - 2.0794415 * jax.random.uniform(seeds[3], (ROWS,), jnp.float32) ** levels(seeds[3], (ROWS,), ((0, 32),), -0.2, 0.2)), 8.0, 64.0)
    vectors = noise(seeds[4], (ROWS, NV), ROWS ** -0.5, 0.09375, ((0, 32),))
    return {"densities": densities, "counts": counts, "coulomb": coulomb, "energies": energies, "vectors": vectors}


def reference(densities, counts, coulomb, energies, vectors):
    slots_idx = lax.broadcasted_iota(jnp.int32, (NK, SLOT), 1)
    usable = (slots_idx < counts[:, None]).reshape(NK * SLOT)
    masked = jnp.where(usable[:, None], densities.astype(jnp.float32), 0.0)
    weighted = lax.optimization_barrier((masked * coulomb[None, :]).astype(jnp.bfloat16)).astype(jnp.float32)
    ordered = masked.reshape(N_ROW, N_COL, K_DEV * SLOT, G).transpose(1, 0, 2, 3).reshape(NK * SLOT, G)
    kernel = jnp.dot(weighted, ordered.T, precision=lax.Precision.HIGHEST, preferred_element_type=jnp.float32)
    projected = jnp.dot(masked.T, vectors.astype(jnp.float32), precision=lax.Precision.HIGHEST, preferred_element_type=jnp.float32)
    coupled = jnp.dot(weighted, projected, precision=lax.Precision.HIGHEST, preferred_element_type=jnp.float32)
    diagonal = jnp.where(usable, energies, 0.0)
    product = coupled + diagonal[:, None] * vectors.astype(jnp.float32)
    return kernel, product
```

```python
import functools

import jax
import jax.numpy as jnp
from jax import lax
from jax.experimental import pallas as pl
from jax.experimental.pallas import tpu as pltpu
from jax.sharding import PartitionSpec as P

SLOT = 9
LANES = 128
MESH = pl.DeviceIdType.MESH
NT = (((1,), (1,)), ((), ()))
NN = (((1,), (0,)), ((), ()))


def pack(v, groups):
    height = v.shape[0] // groups
    tail = jnp.concatenate([v[j * height:(j + 1) * height, LANES:] for j in range(groups)], axis=1)
    spare = LANES - tail.shape[1]
    if spare:
        tail = jnp.concatenate([tail, jnp.zeros((height, spare), v.dtype)], axis=1)
    return jnp.concatenate([v[:, :LANES], tail], axis=0)


def unpack(p, rows, rest, groups):
    tail = jnp.concatenate([p[rows:, j * rest:(j + 1) * rest] for j in range(groups)], axis=0)
    return jnp.concatenate([p[:rows], tail], axis=1)


def groups_of(rows, rest):
    return max(g for g in range(1, LANES // rest + 1) if rows % g == 0 and rows // g % 8 == 0)


def plan(line):
    pairs = [(i, j) for i in range(line) for j in range(i + 1, line)]
    modes = {6: "jjbiii"}.get(len(pairs), "b" * len(pairs))
    computed = [[i] for i in range(line)]
    exports = [[] for _ in range(line)]
    high, low = list(range(line)), list(range(line))
    for (i, j), mode in zip(pairs, modes):
        if mode in "jb":
            computed[j].append(i)
            high[i] = max(high[i], j)
        if mode in "ib":
            computed[i].append(j)
            low[j] = min(low[j], i)
        if mode == "j":
            exports[j].append(i)
        if mode == "i":
            exports[i].append(j)
    special = len(pairs) == 6
    held = [special and low[i] < i and any(low[j] < i for j in range(i + 1, line)) for i in range(line)]
    if special:
        order = [[None, None, 3], [0, 3, 2], [3, 0, None], [None, None, 0]]
    else:
        order = [sorted((j for j in range(line) if j != i), key=lambda j: abs(i - j)) for i in range(line)]
    return computed, exports, high, low, held, order


def look(index, values):
    out = jnp.int32(0)
    for i, value in enumerate(values):
        out = jnp.where(index == i, jnp.int32(value), out)
    return out


def among(a, b, table):
    out = jnp.bool_(False)
    for i, row in enumerate(table):
        for j in row:
            out = out | ((a == i) & (b == j))
    return out


def exchange_kernel(n_row, n_col, chunks, raw_ref, counts_ref, energies_ref, vt_ref, coulomb_ref, out_ref, prod_ref,
                    rows, cols, buf, ysend, tsend, tland, vline, vland, vplane, q, back, bsend, bland, qsend, qland,
                    up_send, down_send, z_recv, xs_send, xf_send, ys_send, yf_send, sib_send, r_recv, s_recv,
                    vp_send, vp_recv, vl_send, vl_recv, yr_send, yr_recv, t_send, t_recv, b_send, b_recv,
                    q_send, q_recv):
    line, chips = n_row // 2, n_col // 2
    computed, exports, high, low, held, order = plan(line)
    special = any(exports)
    r, c = lax.axis_index("row"), lax.axis_index("col")
    z, y = r // 2, lax.rem(r, 2)
    x, core = c // 2, lax.rem(c, 2)
    other_y, other_core = 1 - y, 1 - core
    block, depth = raw_ref.shape
    half = depth // 2
    chunk = block // chunks
    nv = prod_ref.shape[0]
    rest = block % LANES
    vgroups, tgroups = groups_of(nv, rest), groups_of(block, rest)
    place = y * n_col + c
    plane = 2 * n_col
    f32, bf16 = jnp.float32, jnp.bfloat16

    barrier = pltpu.get_barrier_semaphore()
    for step in range(1, plane):
        t = lax.rem(place + step, plane)
        pl.semaphore_signal(barrier, inc=1, device_id=(z * 2 + t // n_col, lax.rem(t, n_col)), device_id_type=MESH)
    for step in range(1, line):
        for cc in range(n_col):
            pl.semaphore_signal(barrier, inc=1, device_id=(lax.rem(z + step, line) * 2 + y, cc), device_id_type=MESH)

    kpoints = counts_ref.shape[1]
    counts = counts_ref[...].astype(f32)
    row_index = lax.broadcasted_iota(jnp.int32, (block, kpoints), 0)
    kpoint = lax.broadcasted_iota(jnp.int32, (block, kpoints), 1)
    slot = row_index - SLOT * kpoint
    inside = (slot >= 0) & (slot < SLOT) & (slot.astype(f32) < counts)
    usable = jnp.sum(jnp.where(inside, 1.0, 0.0), axis=1, keepdims=True)
    d = jnp.where(usable > 0.5, raw_ref[...].astype(f32), 0.0)
    rows[y, c] = d.astype(bf16)
    cols[z] = (d * coulomb_ref[...]).astype(bf16)
    v_mine = pack(vt_ref[...].astype(f32), vgroups).astype(bf16)
    vline[z] = v_mine
    vland[y, c] = v_mine
    pl.semaphore_wait(barrier, plane - 1 + (line - 1) * n_col)

    partner = (z * 2 + other_y, c)
    sibling = (r, x * 2 + other_core)

    def remote(src, dst, send, recv, device):
        return pltpu.make_async_remote_copy(
            src_ref=src, dst_ref=dst, send_sem=send, recv_sem=recv, device_id=device, device_id_type=MESH)

    def piece(zp, ch):
        return cols.at[zp, pl.ds(ch * chunk, chunk)]

    def up(zp, ch):
        return remote(piece(zp, ch), piece(zp, ch), up_send.at[zp, ch], z_recv.at[zp, ch], ((z + 1) * 2 + y, c))

    def down(zp, ch):
        return remote(piece(zp, ch), piece(zp, ch), down_send.at[zp, ch], z_recv.at[zp, ch], ((z - 1) * 2 + y, c))

    def part(yy, cc, h):
        return rows.at[yy, cc, :, pl.ds(h * half, half)]

    def x_peer(step):
        return (r, lax.rem(x + step, chips) * 2 + core)

    def x_own(step, h):
        return remote(part(y, c, h), part(y, c, h), xs_send.at[step, h], r_recv.at[y, x, h], x_peer(step))

    def x_forward(step):
        return remote(part(other_y, c, 1), part(other_y, c, 1), xf_send.at[step], r_recv.at[other_y, x, 1], x_peer(step))

    def y_own(h):
        return remote(part(y, c, h), part(y, c, h), ys_send.at[h], r_recv.at[y, x, h], partner)

    def y_forward(xx):
        cc = xx * 2 + core
        return remote(part(y, cc, 0), part(y, cc, 0), yf_send.at[xx], r_recv.at[y, xx, 0], partner)

    def share(yy, xx, h):
        cc = xx * 2 + core
        return remote(part(yy, cc, h), part(yy, cc, h), sib_send.at[yy, xx, h], s_recv.at[yy, xx, h], sibling)

    def arrive(yy, xx, h):
        cc = xx * 2 + core
        remote(part(yy, cc, h), part(yy, cc, h), sib_send.at[yy, xx, h], r_recv.at[yy, xx, h], sibling).wait_recv()
        share(yy, xx, h).start()

    def shared(yy):
        for xx in range(chips):
            for h in range(2):
                cc = xx * 2 + other_core
                remote(part(yy, cc, h), part(yy, cc, h), sib_send.at[yy, xx, h], s_recv.at[yy, xx, h],
                       sibling).wait_recv()

    goes_up = look(z, [high[i] > i for i in range(line)]) > 0
    goes_down = look(z, [low[i] < i for i in range(line)]) > 0
    holds = look(z, held) > 0

    for ch in range(chunks):
        @pl.when(goes_up)
        def _():
            up(z, ch).start()

        @pl.when(goes_down & (~holds if ch else goes_down))
        def _():
            down(z, ch).start()
    for h in range(2):
        share(y, x, h).start()
        for step in range(1, chips):
            x_own(step, h).start()
        y_own(h).start()

    def v_plane(step):
        t = lax.rem(place + step, plane)
        return remote(vline.at[z], vland.at[y, c], vp_send.at[step], vp_recv.at[place],
                      (z * 2 + t // n_col, lax.rem(t, n_col)))

    def v_line(zt):
        return remote(vline.at[z], vline.at[z], vl_send.at[zt], vl_recv.at[z], (zt * 2 + y, c))

    for step in range(1, plane):
        v_plane(step).start()
    for zt in range(line):
        @pl.when((z != zt) & among(zt, z, computed))
        def _():
            v_line(zt).start()
    q[...] = jnp.zeros_like(q)

    def z_event(h, ch, late=False):
        if not late:
            below = z - h

            @pl.when((below >= 0) & (look(below, high) >= z))
            def _():
                remote(piece(below, ch), piece(below, ch), up_send.at[below, ch], z_recv.at[below, ch],
                       sibling).wait_recv()

                @pl.when(look(below, high) > z)
                def _():
                    up(below, ch).start()
        above = z + h
        mine = (above < line) & (look(above, low) <= z)
        if ch:
            mine = mine & ((look(above, held) > 0) == late)

        @pl.when(mine)
        def _():
            remote(piece(above, ch), piece(above, ch), down_send.at[above, ch], z_recv.at[above, ch],
                   sibling).wait_recv()

            @pl.when(look(above, low) < z)
            def _():
                down(above, ch).start()
        if h == 1 and ch == chunks - 1 and not late:
            for later in range(1, chunks):
                @pl.when(holds)
                def _():
                    down(z, later).start()

    def x_event(h):
        for step in range(1, chips):
            xs = lax.rem(x + chips - step, chips)
            arrive(y, xs, h)
            if h == 0:
                y_forward(xs).start()

    def y_event(h):
        arrive(other_y, x, h)
        if h == 1:
            for step in range(1, chips):
                x_forward(step).start()

    def far_event(h):
        for step in range(1, chips):
            arrive(other_y, lax.rem(x + chips - step, chips), h)

    def y_result(zi):
        return remote(ysend.at[zi], buf.at[zi, y], yr_send.at[zi], yr_recv.at[zi], partner)

    def tile_copy(zi, yy, cc):
        return remote(tsend.at[zi, yy, cc], tland.at[z, yy, c], t_send.at[zi, yy, cc], t_recv.at[z, yy, c],
                      (zi * 2 + y, cc))

    def back_copy(zi):
        return remote(bsend.at[zi], bland.at[z], b_send.at[zi], b_recv.at[z], (zi * 2 + y, c))

    def multiply(zi, near):
        yy = y if near else other_y
        both = rows[yy].reshape(n_col * block, depth)
        tile = lax.dot_general(cols[zi], both, NT, preferred_element_type=f32)
        small = tile.astype(bf16)
        if near:
            own = zi == line
            buf[jnp.where(own, z, zi), jnp.where(own, other_y, y)] = small
        else:
            ysend[zi] = small
            y_result(zi).start()
        if special:
            @pl.when(among(z, zi, exports))
            def _():
                for cc in range(n_col):
                    tsend[zi, yy, cc] = pack(tile[:, cc * block:(cc + 1) * block], tgroups).astype(bf16)
                for cc in range(n_col):
                    tile_copy(zi, yy, cc).start()
                term = lax.dot_general(vplane[yy], small, NT, preferred_element_type=f32)
                if near:
                    back[zi] = term
                else:
                    bsend[zi] = pack(back[zi] + term, vgroups).astype(bf16)
                    back_copy(zi).start()
        v = unpack(vline[zi].astype(f32), nv, rest, vgroups).astype(bf16)
        q[yy] += lax.dot_general(v, small, NN, preferred_element_type=f32)

    def v_wait(zi):
        remote(vline.at[zi], vline.at[zi], vl_send.at[zi], vl_recv.at[zi], sibling).wait_recv()

    ranks = len(order[0])
    rank_of = [[-1 if row[k] is None else row[k] for row in order] for k in range(ranks)]

    def ranked(k, near):
        zi = look(z, rank_of[k])

        @pl.when(zi >= 0)
        def _():
            if near:
                v_wait(zi)
            multiply(zi, near)

    def first(with_rank):
        for yy in range(2):
            for cc in range(n_col):
                source = yy * n_col + cc

                @pl.when(place != source)
                def _():
                    remote(vline.at[0], vland.at[yy, cc], vp_send.at[0], vp_recv.at[source], sibling).wait_recv()
        vline[line] = vland[other_y, c]
        for yy in range(2):
            vplane[yy] = jnp.concatenate(
                [unpack(vland[yy, cc].astype(f32), nv, rest, vgroups) for cc in range(n_col)], axis=1).astype(bf16)
        cols[line] = (rows[other_y, c].astype(f32) * coulomb_ref[...]).astype(bf16)
        extra = look(z, rank_of[0]) if with_rank else jnp.int32(-1)

        def body(t, carry):
            zi = jnp.where(t == 0, z, jnp.where(t == 1, line, extra))

            @pl.when(zi >= 0)
            def _():
                @pl.when(t == 2)
                def _():
                    v_wait(zi)
                multiply(zi, True)
            return carry

        lax.fori_loop(0, 3 if with_rank else 2, body, 0)

    def place_computed(zz):
        @pl.when(among(z, jnp.int32(zz), computed))
        def _():
            @pl.when(z != zz)
            def _():
                remote(ysend.at[zz], buf.at[zz, other_y], yr_send.at[zz], yr_recv.at[zz], partner).wait_recv()
            out_ref[:, 2 * zz * block:2 * (zz + 1) * block] = (
                buf[zz].reshape(2 * block, n_col * block).astype(f32).T.astype(bf16))

    def place_imported(zz):
        @pl.when(among(jnp.int32(zz), z, exports))
        def _():
            for cc in range(n_col):
                tiles = []
                for yy in range(2):
                    remote(tsend.at[0, 0, 0], tland.at[zz, yy, cc], t_send.at[zz, yy, cc], t_recv.at[zz, yy, cc],
                           partner).wait_recv()
                    tiles.append(unpack(tland[zz, yy, cc].astype(f32), block, rest, tgroups))
                out_ref[cc * block:(cc + 1) * block, 2 * zz * block:2 * (zz + 1) * block] = (
                    jnp.concatenate(tiles, axis=1).astype(bf16))

    events = [(h + ch + 0.24 * h, functools.partial(z_event, h, ch)) for h in range(1, line) for ch in range(chunks)]
    wide = chunks / 2
    events += [
        (wide + 0.25, functools.partial(x_event, 0)), (wide + 0.26, functools.partial(y_event, 0)),
        (2 * wide + 0.25, functools.partial(x_event, 1)), (2 * wide + 0.26, functools.partial(y_event, 1)),
        (3 * wide + 0.25, functools.partial(far_event, 0)), (3 * wide + 0.5, functools.partial(far_event, 1)),
    ]
    if special:
        second = 1 + chunks + 0.48
        events += [
            (second - 0.02, lambda: (shared_near(), first(True))),
            (second + 0.01, lambda: ranked(1, True)),
            (3 * wide + 0.51, lambda: shared(other_y)),
            (3 * wide + 0.52, lambda: lax.fori_loop(0, 2, far_pair, 0)),
            (3 * wide + 0.53, lambda: place_self()),
        ]

    def shared_near():
        shared(y)

    def far_pair(t, carry):
        zi = jnp.where(t == 0, look(z, rank_of[0]), look(z, rank_of[1]))

        @pl.when(zi >= 0)
        def _():
            multiply(zi, False)
        return carry

    def place_self():
        for zz in range(line):
            @pl.when(z == zz)
            def _():
                out_ref[:, 2 * zz * block:2 * (zz + 1) * block] = (
                    buf[zz].reshape(2 * block, n_col * block).astype(f32).T.astype(bf16))

    for _, event in sorted(events, key=lambda e: e[0]):
        event()
    if special:
        for ch in range(1, chunks):
            z_event(1, ch, True)
        ranked(2, True)
        ranked(2, False)
    else:
        shared(y)
        shared(other_y)
        first(False)
        place_self()

        def every(t, carry):
            zi = lax.rem(z + 1 + t, line)
            v_wait(zi)
            multiply(zi, True)
            multiply(zi, False)
            return carry

        lax.fori_loop(0, line - 1, every, 0)

    for yy in range(2):
        for cc in range(n_col):
            qsend[yy * n_col + cc] = pack(q[yy][:, cc * block:(cc + 1) * block], vgroups).astype(bf16)

    def q_copy(step):
        t = lax.rem(place + step, plane)
        return remote(qsend.at[t], qland.at[place], q_send.at[step], q_recv.at[place],
                      (z * 2 + t // n_col, lax.rem(t, n_col)))

    for step in range(1, plane):
        q_copy(step).start()

    for zz in range(line):
        @pl.when(z != zz)
        def _():
            place_computed(zz)

    answer = qsend[place].astype(f32)
    for step in range(1, plane):
        source = lax.rem(place + step, plane)
        remote(qsend.at[0], qland.at[source], q_send.at[step], q_recv.at[source], sibling).wait_recv()
        answer += qland[source].astype(f32)
    back[line] = unpack(answer, nv, rest, vgroups)
    for zz in range(line):
        @pl.when(among(jnp.int32(zz), z, exports))
        def _():
            remote(bsend.at[0], bland.at[zz], b_send.at[0], b_recv.at[zz], sibling).wait_recv()
            back[line] += unpack(bland[zz].astype(f32), nv, rest, vgroups)
    lane_slot = (lax.broadcasted_iota(jnp.int32, (kpoints, block), 1)
                 - SLOT * lax.broadcasted_iota(jnp.int32, (kpoints, block), 0))
    mine = jnp.where((lane_slot >= 0) & (lane_slot < SLOT), 1.0, 0.0)
    limit = lax.dot_general(jnp.broadcast_to(counts, (8, kpoints)), mine, NN, preferred_element_type=f32)[:1]
    lane_slot = lax.rem(lax.broadcasted_iota(jnp.int32, (1, block), 1), SLOT).astype(f32)
    diagonal = jnp.where(lane_slot + 0.5 < limit, energies_ref[...], 0.0)
    prod_ref[...] = back[line] + diagonal * vt_ref[...].astype(f32)

    if special:
        for zz in range(line):
            place_imported(zz)

    for ch in range(chunks):
        for zp in range(line):
            @pl.when((zp <= z) & (high[zp] > z))
            def _():
                up(zp, ch).wait_send()

            @pl.when((zp >= z) & (low[zp] < z))
            def _():
                down(zp, ch).wait_send()
    for h in range(2):
        y_own(h).wait_send()
        for step in range(1, chips):
            x_own(step, h).wait_send()
        for yy in range(2):
            for xx in range(chips):
                share(yy, xx, h).wait_send()
    for step in range(1, chips):
        x_forward(step).wait_send()
        y_forward(lax.rem(x + step, chips)).wait_send()
    for step in range(1, plane):
        v_plane(step).wait_send()
        q_copy(step).wait_send()
    for zz in range(line):
        @pl.when((z != zz) & among(jnp.int32(zz), z, computed))
        def _():
            v_line(zz).wait_send()

        @pl.when((z != zz) & among(z, jnp.int32(zz), computed))
        def _():
            y_result(zz).wait_send()

        @pl.when(among(z, jnp.int32(zz), exports))
        def _():
            for yy in range(2):
                for cc in range(n_col):
                    tile_copy(zz, yy, cc).wait_send()
            back_copy(zz).wait_send()


def body(n_row, n_col, densities, counts, coulomb, energies, vectors):
    block, depth = densities.shape
    nv = vectors.shape[1]
    line, chips = n_row // 2, n_col // 2
    plane = 2 * n_col
    chunks = 3
    bf16, f32 = jnp.bfloat16, jnp.float32
    rest = block % LANES
    vrows = nv + nv // groups_of(nv, rest)
    trows = block + block // groups_of(block, rest)
    special = any(plan(line)[1])
    vmem = pl.BlockSpec(memory_space=pltpu.VMEM)
    dma = pltpu.SemaphoreType.DMA
    wide = n_col * block
    tiles = (line, 2, n_col, trows, LANES) if special else (1, 1, 1, trows, LANES)
    kernel, prod = pl.pallas_call(
        functools.partial(exchange_kernel, n_row, n_col, chunks),
        out_shape=(
            jax.ShapeDtypeStruct((wide, n_row * block), bf16),
            jax.ShapeDtypeStruct((nv, block), f32),
        ),
        in_specs=[vmem] * 5,
        out_specs=(vmem, vmem),
        scratch_shapes=[
            pltpu.VMEM((2, n_col, block, depth), bf16),
            pltpu.VMEM((line + 1, block, depth), bf16),
            pltpu.VMEM((line, 2, block, wide), bf16),
            pltpu.VMEM((line, block, wide), bf16),
            pltpu.VMEM(tiles, bf16),
            pltpu.VMEM(tiles, bf16),
            pltpu.VMEM((line + 1, vrows, LANES), bf16),
            pltpu.VMEM((2, n_col, vrows, LANES), bf16),
            pltpu.VMEM((2, nv, wide), bf16),
            pltpu.VMEM((2, nv, wide), f32),
            pltpu.VMEM((line + 1, nv, block), f32),
            pltpu.VMEM((line, vrows, LANES), bf16),
            pltpu.VMEM((line, vrows, LANES), bf16),
            pltpu.VMEM((plane, vrows, LANES), bf16),
            pltpu.VMEM((plane, vrows, LANES), bf16),
            dma((line, chunks)), dma((line, chunks)), dma((line, chunks)),
            dma((chips, 2)), dma((chips,)), dma((2,)), dma((chips,)),
            dma((2, chips, 2)), dma((2, chips, 2)), dma((2, chips, 2)),
            dma((plane,)), dma((plane,)), dma((line,)), dma((line,)),
            dma((line,)), dma((line,)),
            dma((line, 2, n_col)), dma((line, 2, n_col)), dma((line,)), dma((line,)),
            dma((plane,)), dma((plane,)),
        ],
        compiler_params=pltpu.CompilerParams(
            collective_id=0, has_side_effects=True, vmem_limit_bytes=60 * 2**20),
    )(densities, counts[None], energies[None], vectors.T, coulomb[None])
    return (kernel.astype(f32), prod.T)


def solution(mesh):
    return jax.shard_map(
        functools.partial(body, mesh.shape["row"], mesh.shape["col"]),
        mesh=mesh,
        in_specs=(
            P(("row", "col"), None),
            P(("row", "col")),
            P(),
            P(("row", "col")),
            P(("row", "col"), None),
        ),
        out_specs=(P("row", "col"), P(("row", "col"), None)),
        check_vma=False,
    )
```

```python
import functools
import math

import jax
import jax.numpy as jnp
from jax import lax
from jax.experimental import pallas as pl
from jax.experimental.pallas import tpu as pltpu
from jax.sharding import PartitionSpec as P

SLOT = 9
LANES = 128
MESH = pl.DeviceIdType.MESH
NT = (((1,), (1,)), ((), ()))
NN = (((1,), (0,)), ((), ()))


def pack(v, groups):
    height = v.shape[0] // groups
    tail = jnp.concatenate([v[j * height:(j + 1) * height, LANES:] for j in range(groups)], axis=1)
    spare = LANES - tail.shape[1]
    if spare:
        tail = jnp.concatenate([tail, jnp.zeros((height, spare), v.dtype)], axis=1)
    return jnp.concatenate([v[:, :LANES], tail], axis=0)


def unpack(p, rows, rest, groups):
    tail = jnp.concatenate([p[rows:, j * rest:(j + 1) * rest] for j in range(groups)], axis=0)
    return jnp.concatenate([p[:rows], tail], axis=1)


def groups_of(rows, rest):
    return max(g for g in range(1, LANES // rest + 1) if rows % g == 0 and rows // g % 8 == 0)


def plan(line):
    pairs = [(i, j) for i in range(line) for j in range(i + 1, line)]
    modes = {6: "jjbiii"}.get(len(pairs), "b" * len(pairs))
    computed = [[i] for i in range(line)]
    exports = [[] for _ in range(line)]
    high, low = list(range(line)), list(range(line))
    for (i, j), mode in zip(pairs, modes):
        if mode in "jb":
            computed[j].append(i)
            high[i] = max(high[i], j)
        if mode in "ib":
            computed[i].append(j)
            low[j] = min(low[j], i)
        if mode == "j":
            exports[j].append(i)
        if mode == "i":
            exports[i].append(j)
    special = len(pairs) == 6
    held = [special and low[i] < i and any(low[j] < i for j in range(i + 1, line)) for i in range(line)]
    if special:
        order = [[None, 3, None], [0, 3, 2], [3, 0, None], [None, 0, None]]
    else:
        order = [sorted((j for j in range(line) if j != i), key=lambda j: abs(i - j)) for i in range(line)]
    return computed, exports, high, low, held, order


def look(index, values):
    out = jnp.int32(0)
    for i, value in enumerate(values):
        out = jnp.where(index == i, jnp.int32(value), out)
    return out


def among(a, b, table):
    out = jnp.bool_(False)
    for i, row in enumerate(table):
        for j in row:
            out = out | ((a == i) & (b == j))
    return out


def exchange_kernel(n_row, n_col, chunks, parts, raw_hbm, counts_hbm, energies_hbm, vt_hbm, coulomb_hbm, out_ref, prod_ref,
                    raw_ref, counts_ref, energies_ref, vt_ref, coulomb_ref, load_sem,
                    rows, cols, buf, ysend, tsend, tland, vline, vland, vplane, q, back, bsend, bland, qsend, qland,
                    up_send, down_send, z_recv, x_send, xf_send, y_send, yf_send, sib_send, r_recv, s_recv,
                    vp_send, vp_recv, vl_send, vl_recv, yr_send, yr_recv, t_send, t_recv, b_send, b_recv,
                    q_send, q_recv):
    line, chips = n_row // 2, n_col // 2
    computed, exports, high, low, held, order = plan(line)
    special = any(exports)
    r, c = lax.axis_index("row"), lax.axis_index("col")
    z, y = r // 2, lax.rem(r, 2)
    x, core = c // 2, lax.rem(c, 2)
    other_y, other_core = 1 - y, 1 - core
    block, depth = raw_ref.shape
    half = depth // 2
    chunk = block // chunks
    lead = chunks // parts
    sub = block // parts
    nv = prod_ref.shape[0]
    rest = block % LANES
    vgroups, tgroups = groups_of(nv, rest), groups_of(sub, rest)
    place = y * n_col + c
    plane = 2 * n_col
    f32, bf16 = jnp.float32, jnp.bfloat16

    loads = [
        pltpu.make_async_copy(src, dst, load_sem.at[i])
        for i, (src, dst) in enumerate((
            (counts_hbm, counts_ref), (coulomb_hbm, coulomb_ref), (raw_hbm, raw_ref), (vt_hbm, vt_ref),
            (energies_hbm, energies_ref)))
    ]
    for load in loads:
        load.start()
    barrier = pltpu.get_barrier_semaphore()
    for step in range(1, plane):
        t = lax.rem(place + step, plane)
        pl.semaphore_signal(barrier, inc=1, device_id=(z * 2 + t // n_col, lax.rem(t, n_col)), device_id_type=MESH)
    for step in range(1, line):
        for cc in range(n_col):
            pl.semaphore_signal(barrier, inc=1, device_id=(lax.rem(z + step, line) * 2 + y, cc), device_id_type=MESH)

    for load in loads:
        load.wait()
    kpoints = counts_ref.shape[1]
    counts = counts_ref[...].astype(f32)
    row_index = lax.broadcasted_iota(jnp.int32, (block, kpoints), 0)
    kpoint = lax.broadcasted_iota(jnp.int32, (block, kpoints), 1)
    slot = row_index - SLOT * kpoint
    inside = (slot >= 0) & (slot < SLOT) & (slot.astype(f32) < counts)
    usable = jnp.sum(jnp.where(inside, 1.0, 0.0), axis=1, keepdims=True)
    d = jnp.where(usable > 0.5, raw_ref[...].astype(f32), 0.0)
    rows[y, c] = d.astype(bf16)
    cols[z] = (d * coulomb_ref[...]).astype(bf16)
    v_mine = pack(vt_ref[...].astype(f32), vgroups).astype(bf16)
    vline[z] = v_mine
    vland[y, c] = v_mine
    pl.semaphore_wait(barrier, plane - 1 + (line - 1) * n_col)

    partner = (z * 2 + other_y, c)
    sibling = (r, x * 2 + other_core)

    def remote(src, dst, send, recv, device):
        return pltpu.make_async_remote_copy(
            src_ref=src, dst_ref=dst, send_sem=send, recv_sem=recv, device_id=device, device_id_type=MESH)

    def piece(zp, ch):
        return cols.at[zp, pl.ds(ch * chunk, chunk)]

    def up(zp, ch):
        return remote(piece(zp, ch), piece(zp, ch), up_send.at[zp], z_recv.at[zp, ch], ((z + 1) * 2 + y, c))

    def down(zp, ch):
        return remote(piece(zp, ch), piece(zp, ch), down_send.at[zp], z_recv.at[zp, ch], ((z - 1) * 2 + y, c))

    def part(yy, cc, h):
        return rows.at[yy, cc, :, pl.ds(h * half, half)]

    def x_peer(step):
        return (r, lax.rem(x + step, chips) * 2 + core)

    def x_own(step, h):
        return remote(part(y, c, h), part(y, c, h), x_send, r_recv.at[y, x, h], x_peer(step))

    def x_forward(step):
        return remote(part(other_y, c, 1), part(other_y, c, 1), xf_send, r_recv.at[other_y, x, 1], x_peer(step))

    def y_own(h):
        return remote(part(y, c, h), part(y, c, h), y_send, r_recv.at[y, x, h], partner)

    def y_forward(xx):
        cc = xx * 2 + core
        return remote(part(y, cc, 0), part(y, cc, 0), yf_send, r_recv.at[y, xx, 0], partner)

    def share(yy, xx, h):
        cc = xx * 2 + core
        return remote(part(yy, cc, h), part(yy, cc, h), sib_send, s_recv.at[yy], sibling)

    def arrive(yy, xx, h):
        cc = xx * 2 + core
        remote(part(yy, cc, h), part(yy, cc, h), sib_send, r_recv.at[yy, xx, h], sibling).wait_recv()
        share(yy, xx, h).start()

    def shared(yy):
        half_plane = rows.at[yy, pl.ds(0, chips)]
        remote(half_plane, half_plane, sib_send, s_recv.at[yy], sibling).wait_recv()

    goes_up = look(z, [high[i] > i for i in range(line)]) > 0
    goes_down = look(z, [low[i] < i for i in range(line)]) > 0
    holds = look(z, held) > 0

    for ch in range(chunks):
        @pl.when(goes_up)
        def _():
            up(z, ch).start()

        @pl.when(goes_down & (~holds if ch >= lead else goes_down))
        def _():
            down(z, ch).start()
    for h in range(2):
        share(y, x, h).start()
        for step in range(1, chips):
            x_own(step, h).start()
        y_own(1 - h).start()

    def v_plane(step):
        t = lax.rem(place + step, plane)
        return remote(vline.at[z], vland.at[y, c], vp_send, vp_recv,
                      (z * 2 + t // n_col, lax.rem(t, n_col)))

    def v_line(zt):
        return remote(vline.at[z], vline.at[z], vl_send.at[zt], vl_recv.at[z], (zt * 2 + y, c))

    for step in range(1, plane):
        v_plane(step).start()
    for zt in range(line):
        @pl.when((z != zt) & among(zt, z, computed))
        def _():
            v_line(zt).start()
    q[...] = jnp.zeros_like(q)

    def z_event(h, ch, late=False):
        if not late:
            below = z - h

            @pl.when((below >= 0) & (look(below, high) >= z))
            def _():
                remote(piece(below, ch), piece(below, ch), up_send.at[0], z_recv.at[below, ch],
                       sibling).wait_recv()

                @pl.when(look(below, high) > z)
                def _():
                    up(below, ch).start()
        above = z + h
        mine = (above < line) & (look(above, low) <= z)
        if ch >= lead:
            mine = mine & ((look(above, held) > 0) == late)

        @pl.when(mine)
        def _():
            remote(piece(above, ch), piece(above, ch), down_send.at[0], z_recv.at[above, ch],
                   sibling).wait_recv()

            @pl.when(look(above, low) < z)
            def _():
                down(above, ch).start()
        if h == 1 and ch == chunks - 1 and not late:
            for later in range(lead, chunks):
                @pl.when(holds)
                def _():
                    down(z, later).start()

    def x_event(h):
        for step in range(1, chips):
            xs = lax.rem(x + chips - step, chips)
            arrive(y, xs, h)
            if h == 0:
                y_forward(xs).start()

    def y_event(h):
        arrive(other_y, x, h)
        if h == 1:
            for step in range(1, chips):
                x_forward(step).start()

    def far_event(h):
        for step in range(1, chips):
            arrive(other_y, lax.rem(x + chips - step, chips), h)

    def y_result(zi, p):
        rows_of = pl.ds(p * sub, sub)
        return remote(ysend.at[zi, rows_of], buf.at[zi, y, rows_of], yr_send.at[zi], yr_recv.at[zi], partner)

    def tile_copy(zi, yy, cc, p):
        return remote(tsend.at[zi, yy, cc, p], tland.at[z, yy, c, p], t_send.at[zi],
                      t_recv.at[z], (zi * 2 + y, cc))

    def back_copy(zi):
        return remote(bsend.at[zi], bland.at[z], b_send.at[zi], b_recv.at[z], (zi * 2 + y, c))

    def multiply(zi, near, opens=False, closes=False, first_part=0, last_part=parts, sends=True):
        yy = y if near else other_y
        low_row, high_row = first_part * sub, last_part * sub
        both = rows[yy].reshape(n_col * block, depth)
        tile = lax.dot_general(cols[zi, low_row:high_row, :], both, NT, preferred_element_type=f32)
        small = tile.astype(bf16)
        if near:
            own = zi == line
            buf[jnp.where(own, z, zi), jnp.where(own, other_y, y), low_row:high_row] = small
        else:
            ysend[zi, low_row:high_row] = small
            for p in range(first_part, last_part):
                y_result(zi, p).start()
        if special and sends:
            @pl.when(among(z, zi, exports))
            def _():
                for cc in range(n_col):
                    for p in range(first_part, last_part):
                        tsend[zi, yy, cc, p] = pack(
                            tile[(p - first_part) * sub:(p - first_part + 1) * sub, cc * block:(cc + 1) * block],
                            tgroups).astype(bf16)
                for p in range(first_part, last_part):
                    for cc in range(n_col):
                        tile_copy(zi, yy, cc, p).start()
                term = lax.dot_general(vplane[yy], small, NT, preferred_element_type=f32)
                if opens:
                    back[zi, :, low_row:high_row] = term
                else:
                    back[zi, :, low_row:high_row] += term
                if closes:
                    bsend[zi] = pack(back[zi], vgroups).astype(bf16)
                    back_copy(zi).start()
        v = unpack(vline[zi].astype(f32), nv, rest, vgroups)[:, low_row:high_row].astype(bf16)
        q[yy] += lax.dot_general(v, small, NN, preferred_element_type=f32)

    def v_wait(zi):
        remote(vline.at[zi], vline.at[zi], vl_send.at[zi], vl_recv.at[zi], sibling).wait_recv()

    ranks = len(order[0])
    rank_of = [[-1 if row[k] is None else row[k] for row in order] for k in range(ranks)]

    def ranked(k):
        zi = look(z, rank_of[k])

        @pl.when(zi >= 0)
        def _():
            v_wait(zi)
            multiply(zi, True, opens=True)

    def held_parts(first_part, last_part):
        for ch in range(max(lead, first_part * chunks // parts), last_part * chunks // parts):
            z_event(1, ch, True)
        zi = look(z, rank_of[2])

        @pl.when(zi >= 0)
        def _():
            if first_part == 0:
                v_wait(zi)
            multiply(zi, False, opens=True, first_part=first_part, last_part=last_part)
            multiply(zi, True, closes=last_part == parts, first_part=first_part, last_part=last_part)

    def first():
        multiply(z, True, sends=False)

    def second():
        others = qland.at[pl.ds(0, plane - 1)]
        remote(others, others, vp_send, vp_recv, sibling).wait_recv()
        vline[line] = vland[other_y, c]
        for yy in range(2):
            vplane[yy] = jnp.concatenate(
                [unpack(vland[yy, cc].astype(f32), nv, rest, vgroups) for cc in range(n_col)], axis=1).astype(bf16)
        cols[line] = (rows[other_y, c].astype(f32) * coulomb_ref[...]).astype(bf16)
        multiply(jnp.int32(line), True, sends=False)

    def place_computed(zz):
        @pl.when(among(z, jnp.int32(zz), computed))
        def _():
            remote(ysend.at[zz], buf.at[zz, other_y], yr_send.at[zz], yr_recv.at[zz], partner).wait_recv()
            out_ref[:, 2 * zz * block:2 * (zz + 1) * block] = (
                buf[zz].reshape(2 * block, n_col * block).astype(f32).T.astype(bf16))

    def place_imported(zz):
        @pl.when(among(jnp.int32(zz), z, exports))
        def _():
            tiles = []
            remote(tland.at[zz], tland.at[zz], t_send.at[zz], t_recv.at[zz], partner).wait_recv()
            for yy in range(2):
                t = tland[zz, yy].astype(f32).reshape(n_col * parts, tland.shape[4], LANES)
                tail = jnp.concatenate(
                    [t[:, sub:, j * rest:(j + 1) * rest] for j in range(tgroups)], axis=1)
                tiles.append(jnp.concatenate([t[:, :sub], tail], axis=2).reshape(n_col * block, block))
            out_ref[:, 2 * zz * block:2 * (zz + 1) * block] = jnp.concatenate(tiles, axis=1).astype(bf16)

    def shared_near():
        shared(y)

    def far_pair(t, carry):
        zi = jnp.where(t == 0, look(z, rank_of[0]), look(z, rank_of[1]))

        @pl.when(zi >= 0)
        def _():
            multiply(zi, False, closes=True)
        return carry

    def place_self():
        for zz in range(line):
            @pl.when(z == zz)
            def _():
                out_ref[:, 2 * zz * block:2 * (zz + 1) * block] = (
                    buf[zz].reshape(2 * block, n_col * block).astype(f32).T.astype(bf16))

    events = [(0.05 + (ch + h) / chunks + 0.1 * h, functools.partial(z_event, h, ch))
              for h in range(1, line) for ch in range(chunks)]
    events += [
        (0.61, functools.partial(x_event, 0)), (0.62, functools.partial(y_event, 1)),
        (1.11, functools.partial(x_event, 1)), (1.12, functools.partial(y_event, 0)),
        (1.61, functools.partial(far_event, 0)), (1.62, functools.partial(far_event, 1)),
    ]
    if special:
        events += [
            (1.14, shared_near), (1.18, first), (1.37, second),
            (1.38, functools.partial(ranked, 0)), (1.58, functools.partial(ranked, 1)),
            (1.73, functools.partial(shared, other_y)),
            (1.74, lambda: lax.fori_loop(0, 2, far_pair, 0)),
            (1.75, place_self),
        ]

    for _, event in sorted(events, key=lambda e: e[0]):
        event()
    if special:
        held_parts(0, parts - 1)
        held_parts(parts - 1, parts)
    else:
        shared(y)
        shared(other_y)
        first()
        second()
        place_self()

        def every(t, carry):
            zi = lax.rem(z + 1 + t, line)
            v_wait(zi)
            multiply(zi, True)
            multiply(zi, False)
            return carry

        lax.fori_loop(0, line - 1, every, 0)

    for yy in range(2):
        for cc in range(n_col):
            qsend[yy * n_col + cc] = pack(q[yy][:, cc * block:(cc + 1) * block], vgroups).astype(bf16)

    def q_copy(step):
        t = lax.rem(place + step, plane)
        return remote(qsend.at[t], qland.at[place], q_send, q_recv,
                      (z * 2 + t // n_col, lax.rem(t, n_col)))

    for step in range(1, plane):
        q_copy(step).start()

    last = look(z, rank_of[2]) if special else jnp.int32(-1)
    for zz in range(line):
        @pl.when((z != zz) & (last != zz))
        def _():
            place_computed(zz)

    answer = qsend[place].astype(f32)
    others = qland.at[pl.ds(0, plane - 1)]
    remote(others, others, q_send, q_recv, sibling).wait_recv()
    for step in range(1, plane):
        answer += qland[lax.rem(place + step, plane)].astype(f32)
    back[line] = unpack(answer, nv, rest, vgroups)
    if special:
        for zz in range(line):
            place_imported(zz)
    for zz in range(line):
        @pl.when(among(jnp.int32(zz), z, exports))
        def _():
            remote(bsend.at[0], bland.at[zz], b_send.at[0], b_recv.at[zz], sibling).wait_recv()
            back[line] += unpack(bland[zz].astype(f32), nv, rest, vgroups)
    lane_slot = (lax.broadcasted_iota(jnp.int32, (kpoints, block), 1)
                 - SLOT * lax.broadcasted_iota(jnp.int32, (kpoints, block), 0))
    mine = jnp.where((lane_slot >= 0) & (lane_slot < SLOT), 1.0, 0.0)
    limit = lax.dot_general(jnp.broadcast_to(counts, (8, kpoints)), mine, NN, preferred_element_type=f32)[:1]
    lane_slot = lax.rem(lax.broadcasted_iota(jnp.int32, (1, block), 1), SLOT).astype(f32)
    diagonal = jnp.where(lane_slot + 0.5 < limit, energies_ref[...], 0.0)
    prod_ref[...] = back[line] + diagonal * vt_ref[...].astype(f32)

    if special:
        for zz in range(line):
            if zz in rank_of[2]:
                @pl.when(last == zz)
                def _():
                    place_computed(zz)

    def sent(ref, sem):
        remote(ref, ref, sem, load_sem.at[0], sibling).wait_send()

    for zp in range(line):
        @pl.when((zp <= z) & (high[zp] > z))
        def _():
            sent(cols.at[zp], up_send.at[zp])

        @pl.when((zp >= z) & (low[zp] < z))
        def _():
            sent(cols.at[zp], down_send.at[zp])
    sent(rows.at[0, 0], y_send)
    sent(rows.at[0, pl.ds(0, chips - 1)], x_send)
    sent(rows.at[0, pl.ds(0, chips - 1), :, pl.ds(0, half)], xf_send)
    sent(rows.at[0, pl.ds(0, chips - 1), :, pl.ds(0, half)], yf_send)
    sent(rows.at[0], sib_send)
    sent(qland.at[pl.ds(0, plane - 1)], vp_send)
    sent(qland.at[pl.ds(0, plane - 1)], q_send)
    for zz in range(line):
        @pl.when((z != zz) & among(jnp.int32(zz), z, computed))
        def _():
            v_line(zz).wait_send()

        @pl.when((z != zz) & among(z, jnp.int32(zz), computed))
        def _():
            sent(ysend.at[zz], yr_send.at[zz])

        @pl.when(among(z, jnp.int32(zz), exports))
        def _():
            sent(tsend.at[zz], t_send.at[zz])
            back_copy(zz).wait_send()


def body(n_row, n_col, densities, counts, coulomb, energies, vectors):
    block, depth = densities.shape
    nv = vectors.shape[1]
    line, chips = n_row // 2, n_col // 2
    plane = 2 * n_col
    chunks, parts = 9, 3
    bf16, f32 = jnp.bfloat16, jnp.float32
    rest = block % LANES
    vrows = nv + nv // groups_of(nv, rest)
    trows = block // parts + block // parts // groups_of(block // parts, rest)
    special = any(plan(line)[1])
    vmem = pl.BlockSpec(memory_space=pltpu.VMEM)
    dma = pltpu.SemaphoreType.DMA
    wide = n_col * block
    tiles = (line, 2, n_col, parts, trows, LANES) if special else (1, 1, 1, 1, trows, LANES)
    scratch = [
        pltpu.VMEM((block, depth), bf16),
        pltpu.VMEM((1, counts.shape[0]), jnp.int32),
        pltpu.VMEM((1, block), f32),
        pltpu.VMEM((nv, block), bf16),
        pltpu.VMEM((1, depth), f32),
        dma((5,)),
        pltpu.VMEM((2, n_col, block, depth), bf16),
        pltpu.VMEM((line + 1, block, depth), bf16),
        pltpu.VMEM((line, 2, block, wide), bf16),
        pltpu.VMEM((line, block, wide), bf16),
        pltpu.VMEM(tiles, bf16),
        pltpu.VMEM(tiles, bf16),
        pltpu.VMEM((line + 1, vrows, LANES), bf16),
        pltpu.VMEM((2, n_col, vrows, LANES), bf16),
        pltpu.VMEM((2, nv, wide), bf16),
        pltpu.VMEM((2, nv, wide), f32),
        pltpu.VMEM((line + 1, nv, block), f32),
        pltpu.VMEM((line, vrows, LANES), bf16),
        pltpu.VMEM((line, vrows, LANES), bf16),
        pltpu.VMEM((plane, vrows, LANES), bf16),
        pltpu.VMEM((plane, vrows, LANES), bf16),
        dma((line,)), dma((line,)), dma((line, chunks)),
        dma, dma, dma, dma, dma, dma((2, chips, 2)), dma((2,)),
        dma, dma, dma((line,)), dma((line,)),
        dma((line,)), dma((line,)), dma((line,)), dma((line,)), dma((line,)), dma((line,)),
        dma, dma,
    ]
    held = sum(math.prod(ref.shape[:-1]) * -(-ref.shape[-1] // LANES) * LANES * jnp.dtype(ref.dtype).itemsize
               for ref in scratch if getattr(ref, 'dtype', None) in (bf16, f32))
    kernel, prod = pl.pallas_call(
        functools.partial(exchange_kernel, n_row, n_col, chunks, parts),
        out_shape=(
            jax.ShapeDtypeStruct((wide, n_row * block), bf16),
            jax.ShapeDtypeStruct((nv, block), f32),
        ),
        in_specs=[pl.BlockSpec(memory_space=pltpu.MemorySpace.HBM)] * 5,
        out_specs=(vmem, vmem),
        scratch_shapes=scratch,
        compiler_params=pltpu.CompilerParams(
            collective_id=0, has_side_effects=True, vmem_limit_bytes=min(60 * 2**20, held + held // 8 + 6 * 2**20)),
    )(*(pltpu.with_memory_space_constraint(operand, pltpu.MemorySpace.HBM)
        for operand in (densities, counts[None], energies[None], vectors.T, coulomb[None])))
    return (kernel.astype(f32), prod.T)


def solution(mesh):
    return jax.shard_map(
        functools.partial(body, mesh.shape["row"], mesh.shape["col"]),
        mesh=mesh,
        in_specs=(
            P(("row", "col"), None),
            P(("row", "col")),
            P(),
            P(("row", "col")),
            P(("row", "col"), None),
        ),
        out_specs=(P("row", "col"), P(("row", "col"), None)),
        check_vma=False,
    )
```

```python
import functools
import math

import jax
import jax.numpy as jnp
from jax import lax
from jax.experimental import pallas as pl
from jax.experimental.pallas import tpu as pltpu
from jax.sharding import PartitionSpec as P

SLOT = 9
LANES = 128
COPIES = 4
MESH = pl.DeviceIdType.MESH
NT = (((1,), (1,)), ((), ()))
NN = (((1,), (0,)), ((), ()))


def pack(v, groups):
    height = v.shape[0] // groups
    tail = jnp.concatenate([v[j * height:(j + 1) * height, LANES:] for j in range(groups)], axis=1)
    spare = LANES - tail.shape[1]
    if spare:
        tail = jnp.concatenate([tail, jnp.zeros((height, spare), v.dtype)], axis=1)
    return jnp.concatenate([v[:, :LANES], tail], axis=0)


def unpack(p, rows, rest, groups):
    tail = jnp.concatenate([p[rows:, j * rest:(j + 1) * rest] for j in range(groups)], axis=0)
    return jnp.concatenate([p[:rows], tail], axis=1)


def groups_of(rows, rest):
    return max(g for g in range(1, LANES // rest + 1) if rows % g == 0 and rows // g % 8 == 0)


def plan(line):
    pairs = [(i, j) for i in range(line) for j in range(i + 1, line)]
    modes = {6: "jjbiii"}.get(len(pairs), "b" * len(pairs))
    computed = [[i] for i in range(line)]
    exports = [[] for _ in range(line)]
    high, low = list(range(line)), list(range(line))
    for (i, j), mode in zip(pairs, modes):
        if mode in "jb":
            computed[j].append(i)
            high[i] = max(high[i], j)
        if mode in "ib":
            computed[i].append(j)
            low[j] = min(low[j], i)
        if mode == "j":
            exports[j].append(i)
        if mode == "i":
            exports[i].append(j)
    special = len(pairs) == 6
    held = [special and low[i] < i and any(low[j] < i for j in range(i + 1, line)) for i in range(line)]
    order = [[None, 3], [2, None], [None, None], [None, 0]] if special else [[None, None]] * line
    slots = [0, 2, 3, 1] if special else list(range(line))
    return computed, exports, high, low, held, order, slots


def look(index, values):
    out = jnp.int32(0)
    for i, value in enumerate(values):
        out = jnp.where(index == i, jnp.int32(value), out)
    return out


def among(a, b, table):
    out = jnp.bool_(False)
    for i, row in enumerate(table):
        for j in row:
            out = out | ((a == i) & (b == j))
    return out


def exchange_kernel(n_row, n_col, chunks, parts, raw_hbm, counts_hbm, energies_hbm, vt_hbm, coulomb_hbm, out_ref, prod_ref,
                    raw_ref, counts_ref, energies_ref, vt_ref, coulomb_ref, load_sem,
                    rows, w_ref, cols, buf, tsend, tland, yland, vline, vland, vplane, vchip, q, qfar, back, bsend, bland, qsend, qland,
                    up_send, down_send, z_recv, x_send, xf_send, y_send, yf_send, sib_send, r_recv, s_recv,
                    vp_send, vp_recv, vl_send, vl_recv, yr_send, yr_recv, t_send, t_recv, b_send, b_recv,
                    q_send, q_recv):
    line, chips = n_row // 2, n_col // 2
    computed, exports, high, low, held, order, slots = plan(line)
    special = any(exports)
    r, c = lax.axis_index("row"), lax.axis_index("col")
    z, y = line - 1 - r // 2, lax.rem(r, 2)
    x, core = c // 2, lax.rem(c, 2)
    other_y, other_core = 1 - y, 1 - core
    block, depth = raw_ref.shape
    half = depth // 2
    chunk = block // chunks
    lead = chunks // 4
    sub = block // parts
    nv = prod_ref.shape[0]
    rest = block % LANES
    vgroups, tgroups = groups_of(nv, rest), groups_of(sub, rest)
    place = y * n_col + c
    plane = 2 * n_col
    f32, bf16 = jnp.float32, jnp.bfloat16

    loads = [
        pltpu.make_async_copy(src, dst, load_sem.at[i])
        for i, (src, dst) in enumerate((
            (counts_hbm, counts_ref), (coulomb_hbm, coulomb_ref), (raw_hbm, raw_ref), (vt_hbm, vt_ref),
            (energies_hbm, energies_ref)))
    ]
    for load in loads:
        load.start()
    def row_of(zp, yy):
        return (line - 1 - zp) * 2 + yy

    barrier = pltpu.get_barrier_semaphore()
    for step in range(1, plane):
        t = lax.rem(place + step, plane)
        pl.semaphore_signal(barrier, inc=1, device_id=(row_of(z, t // n_col), lax.rem(t, n_col)), device_id_type=MESH)
    for step in range(1, line):
        for cc in range(n_col):
            pl.semaphore_signal(barrier, inc=1, device_id=(row_of(lax.rem(z + step, line), y), cc), device_id_type=MESH)

    for load in loads:
        load.wait()
    kpoints = counts_ref.shape[1]
    counts = counts_ref[...].astype(f32)
    row_index = lax.broadcasted_iota(jnp.int32, (block, kpoints), 0)
    kpoint = lax.broadcasted_iota(jnp.int32, (block, kpoints), 1)
    slot = row_index - SLOT * kpoint
    inside = (slot >= 0) & (slot < SLOT) & (slot.astype(f32) < counts)
    usable = jnp.sum(jnp.where(inside, 1.0, 0.0), axis=1, keepdims=True)
    d = jnp.where(usable > 0.5, raw_ref[...].astype(f32), 0.0)
    rows[y, c] = d.astype(bf16)
    w_ref[0] = (d * coulomb_ref[...]).astype(bf16)
    v_mine = pack(vt_ref[...].astype(f32), vgroups).astype(bf16)
    vline[z] = v_mine
    vland[y, c] = v_mine
    pl.semaphore_wait(barrier, plane - 1 + (line - 1) * n_col)

    partner = (row_of(z, other_y), c)
    sibling = (r, x * 2 + other_core)

    def remote(src, dst, send, recv, device):
        return pltpu.make_async_remote_copy(
            src_ref=src, dst_ref=dst, send_sem=send, recv_sem=recv, device_id=device, device_id_type=MESH)

    def slot_of(zp):
        return look(zp, slots)

    def piece(zp, ch):
        return cols.at[slot_of(zp), pl.ds(ch * chunk, chunk)]

    def relay(zp, ch, step):
        send = up_send if step > 0 else down_send
        src = piece(zp, ch)
        remote(src, src, send.at[zp], z_recv.at[zp, ch], (row_of(z + step, y), c)).start()

    def launch(ch, step):
        send = up_send if step > 0 else down_send
        remote(w_ref.at[0, pl.ds(ch * chunk, chunk)], piece(z, ch), send.at[z], z_recv.at[z, ch],
               (row_of(z + step, y), c)).start()

    def part(yy, cc, h):
        return rows.at[yy, cc, :, pl.ds(h * half, half)]

    def x_peer(step):
        return (r, lax.rem(x + step, chips) * 2 + core)

    def x_own(step, h):
        return remote(part(y, c, h), part(y, c, h), x_send, r_recv.at[y, x, h], x_peer(step))

    def x_forward(step):
        return remote(part(other_y, c, 1), part(other_y, c, 1), xf_send, r_recv.at[other_y, x, 1], x_peer(step))

    def y_own(h):
        return remote(part(y, c, h), part(y, c, h), y_send, r_recv.at[y, x, h], partner)

    def y_forward(xx):
        cc = xx * 2 + core
        return remote(part(y, cc, 0), part(y, cc, 0), yf_send, r_recv.at[y, xx, 0], partner)

    def share(yy, xx, h, group):
        cc = xx * 2 + core
        return remote(part(yy, cc, h), part(yy, cc, h), sib_send, s_recv.at[group], sibling)

    def arrive(yy, xx, h, group):
        cc = xx * 2 + core
        remote(part(yy, cc, h), part(yy, cc, h), sib_send, r_recv.at[yy, xx, h], sibling).wait_recv()
        share(yy, xx, h, group).start()

    def shared(group):
        blocks = rows.at[0, pl.ds(0, (chips, 1, chips - 1)[group])]
        remote(blocks, blocks, sib_send, s_recv.at[group], sibling).wait_recv()

    goes_up = look(z, [high[i] > i for i in range(line)]) > 0
    goes_down = look(z, [low[i] < i for i in range(line)]) > 0
    holds = look(z, held) > 0

    for ch in range(chunks):
        @pl.when(goes_up)
        def _():
            launch(ch, 1)

        @pl.when(goes_down & (~holds if ch >= lead else goes_down))
        def _():
            launch(ch, -1)
    for h in range(2):
        share(y, x, h, 0).start()
        for step in range(1, chips):
            x_own(step, h).start()
        y_own(1 - h).start()

    def v_plane(step):
        t = lax.rem(place + step, plane)
        return remote(vline.at[z], vland.at[y, c], vp_send, vp_recv,
                      (row_of(z, t // n_col), lax.rem(t, n_col)))

    def v_line(zt):
        return remote(vline.at[z], vline.at[z], vl_send.at[zt], vl_recv.at[z], (row_of(zt, y), c))

    for step in range(1, plane):
        v_plane(step).start()
    for zt in range(line):
        @pl.when((z != zt) & among(zt, z, computed))
        def _():
            v_line(zt).start()
    q[...] = jnp.zeros_like(q)
    qfar[...] = jnp.zeros_like(qfar)

    def z_event(h, ch, late=False):
        if not late:
            below = z - h

            @pl.when((below >= 0) & (look(below, high) >= z))
            def _():
                remote(piece(below, ch), piece(below, ch), up_send.at[0], z_recv.at[below, ch],
                       sibling).wait_recv()

                @pl.when(look(below, high) > z)
                def _():
                    relay(below, ch, 1)
        above = z + h
        mine = (above < line) & (look(above, low) <= z)
        if ch >= lead:
            mine = mine & ((look(above, held) > 0) == late)

        @pl.when(mine)
        def _():
            remote(piece(above, ch), piece(above, ch), down_send.at[0], z_recv.at[above, ch],
                   sibling).wait_recv()

            @pl.when(look(above, low) < z)
            def _():
                relay(above, ch, -1)
        if h == 1 and ch == chunks - 1 and not late:
            for later in range(lead, chunks):
                @pl.when(holds)
                def _():
                    launch(later, -1)

    def x_event(h):
        for step in range(1, chips):
            xs = lax.rem(x + chips - step, chips)
            arrive(y, xs, h, 0)
            if h == 0:
                y_forward(xs).start()

    def y_event(h):
        arrive(other_y, x, h, 1)
        if h == 1:
            for step in range(1, chips):
                x_forward(step).start()

    def far_event(h):
        for step in range(1, chips):
            arrive(other_y, lax.rem(x + chips - step, chips), h, 2)

    def y_result(zi, cc, first_part=0, last_part=parts):
        mine = pl.ds(first_part, last_part - first_part)
        return remote(tsend.at[zi, other_y, cc, mine], yland.at[zi, cc, mine], yr_send.at[zi], yr_recv.at[zi], partner)

    def tile_copy(zi, yy, cc, first_part=0, last_part=parts):
        mine = pl.ds(first_part, last_part - first_part)
        return remote(tsend.at[zi, yy, cc, mine], tland.at[z, yy, c, mine], t_send.at[zi], t_recv.at[z],
                      (row_of(zi, y), cc))

    def back_copy(zi):
        return remote(bsend.at[zi], bland.at[z], b_send.at[zi], b_recv.at[z], (row_of(zi, y), c))

    def emit(zi, near, tile, chip=None, opens=False, closes=False, first_part=0, last_part=parts, sends=True,
             starts=True):
        yy = y if near else other_y
        low_row, high_row = first_part * sub, last_part * sub
        small = tile.astype(bf16)
        mine = range(n_col) if chip is None else [chip * 2, chip * 2 + 1]
        if near:
            buf[zi, low_row:high_row] = small
        if sends or not near:
            for i, cc in enumerate(mine):
                for p in range(first_part, last_part):
                    tsend[zi, yy, cc, p] = pack(
                        tile[(p - first_part) * sub:(p - first_part + 1) * sub, i * block:(i + 1) * block],
                        tgroups).astype(bf16)
        if not near:
            for cc in mine:
                y_result(zi, cc, first_part, last_part).start()
        v = unpack(vline[zi].astype(f32), nv, rest, vgroups)[:, low_row:high_row].astype(bf16)
        if sends:
            for cc in mine if starts else ():
                tile_copy(zi, yy, cc, first_part, last_part).start()
            vectors = vplane[yy] if chip is None else vchip[chip]
            term = lax.dot_general(vectors, small, NT, preferred_element_type=f32)
            if opens:
                back[zi, :, low_row:high_row] = term
            else:
                back[zi, :, low_row:high_row] += term
            if closes:
                bsend[zi] = pack(back[zi], vgroups).astype(bf16)
                back_copy(zi).start()
        term = lax.dot_general(v, small, NN, preferred_element_type=f32)
        if near:
            q[...] += term
        elif chip is None:
            for xx in range(chips):
                qfar[xx] += term[:, 2 * xx * block:2 * (xx + 1) * block]
        else:
            qfar[chip] += term

    def plane_rows(yy, chip=None):
        if chip is None:
            return rows[yy].reshape(n_col * block, depth)
        return rows[yy, pl.ds(chip * 2, 2)].reshape(2 * block, depth)

    def multiply(zi, near, first_part=0, last_part=parts, **how):
        tile = lax.dot_general(cols[slot_of(zi), first_part * sub:last_part * sub, :], plane_rows(y if near else other_y),
                               NT, preferred_element_type=f32)
        emit(zi, near, tile, first_part=first_part, last_part=last_part, **how)

    def ends(near, chip=None, opens=False, closes=False):
        @pl.when((z > 0) & (z < line - 1))
        def _():
            if opens:
                v_wait(0)
                v_wait(line - 1)
            tile = lax.dot_general(cols[0:2].reshape(2 * block, depth), plane_rows(y if near else other_y, chip), NT,
                                   preferred_element_type=f32)
            for i, zi in enumerate((0, line - 1)):
                emit(zi, near, tile[i * block:(i + 1) * block], chip=chip, opens=opens, closes=closes,
                     starts=closes or zi == 0)

    def late_tiles():
        @pl.when((z > 0) & (z < line - 1))
        def _():
            for i in range(2):
                tile_copy(line - 1, other_y, x * 2 + i).start()
            for cc in range(n_col):
                tile_copy(line - 1, y, cc).start()

    def v_wait(zi):
        remote(vline.at[zi], vline.at[zi], vl_send.at[zi], vl_recv.at[zi], sibling).wait_recv()

    rank_of = [[-1 if row[k] is None else row[k] for row in order] for k in range(2)]

    def held_parts(first_part, last_part):
        for ch in range(max(lead, first_part * chunks // parts), last_part * chunks // parts):
            z_event(1, ch, True)
        zi = look(z, rank_of[0])

        @pl.when(zi >= 0)
        def _():
            if first_part == 0:
                v_wait(zi)
            multiply(zi, False, opens=True, first_part=first_part, last_part=last_part)
            multiply(zi, True, closes=last_part == parts, first_part=first_part, last_part=last_part)

    def plane_vectors():
        others = qland.at[pl.ds(0, plane - 1)]
        remote(others, others, vp_send, vp_recv, sibling).wait_recv()
        for yy in range(2):
            vplane[yy] = jnp.concatenate(
                [unpack(vland[yy, cc].astype(f32), nv, rest, vgroups) for cc in range(n_col)], axis=1).astype(bf16)
        for xx in range(chips):
            vchip[xx] = jnp.concatenate(
                [unpack(vland[other_y, 2 * xx + i].astype(f32), nv, rest, vgroups) for i in range(2)], axis=1).astype(bf16)
    def own_plane():
        w_ref[1] = (rows[other_y, c].astype(f32) * coulomb_ref[...]).astype(bf16)
        tile = lax.dot_general(w_ref[...].reshape(2 * block, depth), plane_rows(y), NT, preferred_element_type=f32)
        small = tile.astype(bf16)
        buf[z] = small[:block]
        buf[line] = small[block:]
        v = jnp.concatenate(
            [unpack(ref.astype(f32), nv, rest, vgroups) for ref in (vline[z], vland[other_y, c])], axis=1).astype(bf16)
        q[...] += lax.dot_general(v, small, NN, preferred_element_type=f32)

    def arrange(ref):
        t = ref[...].astype(f32).reshape(n_col * parts, ref.shape[-2], LANES)
        tail = jnp.concatenate([t[:, sub:, j * rest:(j + 1) * rest] for j in range(tgroups)], axis=1)
        return jnp.concatenate([t[:, :sub], tail], axis=2).reshape(n_col * block, block)

    def lanes_of(zz):
        return slice(2 * (line - 1 - zz) * block, 2 * (line - zz) * block)

    def place_pair(zz, near, far):
        first, second = jnp.where(y == 0, near, far), jnp.where(y == 0, far, near)
        out_ref[:, lanes_of(zz)] = jnp.concatenate([first, second], axis=0).T

    def place_computed(zz):
        @pl.when(among(z, jnp.int32(zz), computed))
        def _():
            remote(yland.at[zz], yland.at[zz], yr_send.at[zz], yr_recv.at[zz], partner).wait_recv()
            t = arrange(yland.at[zz]).reshape(n_col, block, block)
            far = jnp.concatenate([t[cc] for cc in range(n_col)], axis=1)
            place_pair(zz, buf[zz].astype(f32), far)

    def place_imported(zz):
        @pl.when(among(jnp.int32(zz), z, exports))
        def _():
            remote(tland.at[zz], tland.at[zz], t_send.at[zz], t_recv.at[zz], partner).wait_recv()
            out_ref[:, lanes_of(zz)] = jnp.concatenate(
                [arrange(tland.at[zz, yy]) for yy in range(2)], axis=1)

    def edge(first_part, last_part):
        zi = look(z, rank_of[1])

        @pl.when(zi >= 0)
        def _():
            if first_part == 0:
                v_wait(zi)
            multiply(zi, False, first_part, last_part, sends=False)
            multiply(zi, True, first_part, last_part, sends=False)

    def place_self():
        for zz in range(line):
            @pl.when(z == zz)
            def _():
                place_pair(zz, buf[zz].astype(f32), buf[line].astype(f32))

    def own_at(outer):
        at_end = (z == 0) | (z == line - 1)

        @pl.when(at_end if outer else ~at_end)
        def _():
            own_plane()
            place_self()

    def z_time(h, ch):
        if special and h == line - 1:
            return 1.8 if ch < (parts - 1) * chunks // parts else 1.82
        return 0.05 + (ch + h) / chunks + 0.1 * h + (0.1 if h > 1 else 0.0)

    events = [(z_time(h, ch), functools.partial(z_event, h, ch)) for h in range(1, line) for ch in range(chunks)]
    events += [
        (0.61, functools.partial(x_event, 0)), (0.62, functools.partial(y_event, 1)),
        (1.11, functools.partial(x_event, 1)), (1.12, functools.partial(y_event, 0)),
        (1.61, functools.partial(far_event, 0)), (1.62, functools.partial(far_event, 1)),
    ]
    if special:
        events += [
            (1.18, functools.partial(shared, 0)), (1.499, functools.partial(shared, 1)), (1.185, plane_vectors), (1.19, lambda: own_at(True)), (1.5, lambda: ends(False, x, opens=True)), (1.501, functools.partial(ends, True)),
            (1.503, late_tiles), (1.73, functools.partial(shared, 2)), (1.74, lambda: ends(False, 1 - x, closes=True)),
            (1.81, lambda: edge(0, parts - 1)), (1.83, lambda: edge(parts - 1, parts)),
        ]

    for _, event in sorted(events, key=lambda e: e[0]):
        event()
    if special:
        held_parts(0, parts - 1)
        own_at(False)
        held_parts(parts - 1, parts)
    else:
        for group in range(3):
            shared(group)
        plane_vectors()
        own_plane()
        place_self()

        def every(t, carry):
            zi = lax.rem(z + 1 + t, line)
            v_wait(zi)
            multiply(zi, True, sends=False)
            multiply(zi, False, sends=False)
            return carry

        lax.fori_loop(0, line - 1, every, 0)

    for cc in range(n_col):
        qsend[y * n_col + cc] = pack(q[:, cc * block:(cc + 1) * block], vgroups).astype(bf16)
        low_lane = cc % 2 * block
        qsend[other_y * n_col + cc] = pack(qfar[cc // 2, :, low_lane:low_lane + block], vgroups).astype(bf16)

    def q_copy(step):
        t = lax.rem(place + step, plane)
        return remote(qsend.at[t], qland.at[place], q_send, q_recv,
                      (row_of(z, t // n_col), lax.rem(t, n_col)))

    for step in range(1, plane):
        q_copy(step).start()

    last = look(z, rank_of[0])
    for zz in range(line):
        @pl.when((z != zz) & (last != zz))
        def _():
            place_computed(zz)

    if special:
        for zz in range(line):
            place_imported(zz)
        for zz in range(line):
            if zz in rank_of[0]:
                @pl.when(last == zz)
                def _():
                    place_computed(zz)

    answer = qsend[place].astype(f32)
    others = qland.at[pl.ds(0, plane - 1)]
    remote(others, others, q_send, q_recv, sibling).wait_recv()
    for step in range(1, plane):
        answer += qland[lax.rem(place + step, plane)].astype(f32)
    back[line] = unpack(answer, nv, rest, vgroups)
    for zz in range(line):
        @pl.when(among(jnp.int32(zz), z, exports))
        def _():
            remote(bsend.at[0], bland.at[zz], b_send.at[0], b_recv.at[zz], sibling).wait_recv()
            back[line] += unpack(bland[zz].astype(f32), nv, rest, vgroups)
    lane_slot = (lax.broadcasted_iota(jnp.int32, (kpoints, block), 1)
                 - SLOT * lax.broadcasted_iota(jnp.int32, (kpoints, block), 0))
    mine = jnp.where((lane_slot >= 0) & (lane_slot < SLOT), 1.0, 0.0)
    limit = lax.dot_general(jnp.broadcast_to(counts, (8, kpoints)), mine, NN, preferred_element_type=f32)[:1]
    lane_slot = lax.rem(lax.broadcasted_iota(jnp.int32, (1, block), 1), SLOT).astype(f32)
    diagonal = jnp.where(lane_slot + 0.5 < limit, energies_ref[...], 0.0)
    prod_ref[...] = back[line] + diagonal * vt_ref[...].astype(f32)

    def sent(ref, sem):
        remote(ref, ref, sem, load_sem.at[0], sibling).wait_send()

    for zp in range(line):
        @pl.when((zp <= z) & (high[zp] > z))
        def _():
            sent(cols.at[zp], up_send.at[zp])

        @pl.when((zp >= z) & (low[zp] < z))
        def _():
            sent(cols.at[zp], down_send.at[zp])
    sent(rows.at[0, 0], y_send)
    sent(rows.at[0, pl.ds(0, chips - 1)], x_send)
    sent(rows.at[0, pl.ds(0, chips - 1), :, pl.ds(0, half)], xf_send)
    sent(rows.at[0, pl.ds(0, chips - 1), :, pl.ds(0, half)], yf_send)
    sent(rows.at[0], sib_send)
    sent(qland.at[pl.ds(0, plane - 1)], vp_send)
    sent(qland.at[pl.ds(0, plane - 1)], q_send)
    for zz in range(line):
        @pl.when((z != zz) & among(jnp.int32(zz), z, computed))
        def _():
            v_line(zz).wait_send()

        @pl.when((z != zz) & among(z, jnp.int32(zz), computed))
        def _():
            sent(yland.at[zz], yr_send.at[zz])

        @pl.when(among(z, jnp.int32(zz), exports))
        def _():
            sent(tsend.at[zz], t_send.at[zz])
            back_copy(zz).wait_send()


def write_kernel(kernel_ref, prod_ref, kernel_out, prod_out, sem):
    height = kernel_ref.shape[0] // COPIES
    copies = [pltpu.make_async_copy(prod_ref, prod_out, sem.at[COPIES])]
    for i in range(COPIES):
        part = pl.ds(i * height, height)
        copies.append(pltpu.make_async_copy(kernel_ref.at[part], kernel_out.at[part], sem.at[i]))
    for copy in copies:
        copy.start()
    for copy in copies:
        copy.wait()


def body(n_row, n_col, densities, counts, coulomb, energies, vectors):
    block, depth = densities.shape
    nv = vectors.shape[1]
    line, chips = n_row // 2, n_col // 2
    plane = 2 * n_col
    chunks, parts = 9, 3
    bf16, f32 = jnp.bfloat16, jnp.float32
    rest = block % LANES
    vrows = nv + nv // groups_of(nv, rest)
    trows = block // parts + block // parts // groups_of(block // parts, rest)
    special = any(plan(line)[1])
    vmem = pl.BlockSpec(memory_space=pltpu.VMEM)
    dma = pltpu.SemaphoreType.DMA
    wide = n_col * block
    scratch = [
        pltpu.VMEM((block, depth), bf16),
        pltpu.VMEM((1, counts.shape[0]), jnp.int32),
        pltpu.VMEM((1, block), f32),
        pltpu.VMEM((nv, block), bf16),
        pltpu.VMEM((1, depth), f32),
        dma((5,)),
        pltpu.VMEM((2, n_col, block, depth), bf16),
        pltpu.VMEM((2, block, depth), bf16),
        pltpu.VMEM((line, block, depth), bf16),
        pltpu.VMEM((line + 1, block, wide), bf16),
        pltpu.VMEM((line, 2, n_col, parts, trows, LANES), bf16),
        pltpu.VMEM((line if special else 1, 2, n_col, parts, trows, LANES), bf16),
        pltpu.VMEM((line, n_col, parts, trows, LANES), bf16),
        pltpu.VMEM((line, vrows, LANES), bf16),
        pltpu.VMEM((2, n_col, vrows, LANES), bf16),
        pltpu.VMEM((2, nv, wide), bf16),
        pltpu.VMEM((chips, nv, 2 * block), bf16),
        pltpu.VMEM((nv, wide), f32),
        pltpu.VMEM((chips, nv, 2 * block), f32),
        pltpu.VMEM((line + 1, nv, block), f32),
        pltpu.VMEM((line, vrows, LANES), bf16),
        pltpu.VMEM((line, vrows, LANES), bf16),
        pltpu.VMEM((plane, vrows, LANES), bf16),
        pltpu.VMEM((plane, vrows, LANES), bf16),
        dma((line,)), dma((line,)), dma((line, chunks)),
        dma, dma, dma, dma, dma, dma((2, chips, 2)), dma((3,)),
        dma, dma, dma((line,)), dma((line,)),
        dma((line,)), dma((line,)), dma((line,)), dma((line,)), dma((line,)), dma((line,)),
        dma, dma,
    ]
    held = sum(math.prod(ref.shape[:-1]) * -(-ref.shape[-1] // LANES) * LANES * jnp.dtype(ref.dtype).itemsize
               for ref in scratch if getattr(ref, 'dtype', None) in (bf16, f32))
    result = wide * n_row * block * 4
    kernel, prod = pl.pallas_call(
        functools.partial(exchange_kernel, n_row, n_col, chunks, parts),
        out_shape=(
            jax.ShapeDtypeStruct((wide, n_row * block), f32),
            jax.ShapeDtypeStruct((nv, block), f32),
        ),
        in_specs=[pl.BlockSpec(memory_space=pltpu.MemorySpace.HBM)] * 5,
        out_specs=(vmem, vmem),
        scratch_shapes=scratch,
        compiler_params=pltpu.CompilerParams(
            collective_id=0, has_side_effects=True, vmem_limit_bytes=min(60 * 2**20, held + held // 8 + result + 4 * 2**20)),
    )(*(pltpu.with_memory_space_constraint(operand, pltpu.MemorySpace.HBM)
        for operand in (densities, counts[None], energies[None], vectors.T, coulomb[None])))
    kernel, prod = pl.pallas_call(
        write_kernel,
        out_shape=(
            jax.ShapeDtypeStruct(kernel.shape, f32),
            jax.ShapeDtypeStruct(prod.shape, f32),
        ),
        in_specs=[vmem] * 2,
        out_specs=[pl.BlockSpec(memory_space=pltpu.MemorySpace.HBM)] * 2,
        scratch_shapes=[dma((COPIES + 1,))],
        compiler_params=pltpu.CompilerParams(vmem_limit_bytes=result + 4 * 2**20),
    )(kernel, prod)
    return (kernel, prod.T)


def solution(mesh):
    return jax.shard_map(
        functools.partial(body, mesh.shape["row"], mesh.shape["col"]),
        mesh=mesh,
        in_specs=(
            P(("row", "col"), None),
            P(("row", "col")),
            P(),
            P(("row", "col")),
            P(("row", "col"), None),
        ),
        out_specs=(P("row", "col"), P(("row", "col"), None)),
        check_vma=False,
    )
```
